256 devices in a mesh: rep: 4 (over x, y), ctx: 64 (over z, core).
Axes of the slice: x: 2, y: 2, z: 32, core: 2. Of those that a mesh axis runs over, the one named last changes fastest.
The devices are a block of a 4x8x32 slice.
Arguments:
- queries: bfloat16 [32768, 32, 128], P(('rep', 'ctx')), parts along dimension 0, may hold values from -128 to 128
- keys: bfloat16 [32768, 2, 128], P(('rep', 'ctx')), parts along dimension 0, may hold values from -5 to 5
- values: bfloat16 [32768, 2, 128], P(('rep', 'ctx')), parts along dimension 0, may hold values from -6 to 6
- grad_out: bfloat16 [32768, 32, 128], P(('rep', 'ctx')), parts along dimension 0, may hold values from -6 to 6
- selected: int32 [32768, 2, 8], P(('rep', 'ctx')), parts along dimension 0, may hold values from 0 to 127, as said below
Outputs:
- dquery: bfloat16 [32768, 32, 128], P(('rep', 'ctx')), parts along dimension 0
- key_grad: bfloat16 [32768, 2, 128], P(('rep', 'ctx')), parts along dimension 0
- value_grad: bfloat16 [32768, 2, 128], P(('rep', 'ctx')), parts along dimension 0
The draws below stay inside these ranges and needn't reach their ends.
There are 4 independent parts, one for each index of `rep`. The reference program is written for one: setup_inputs(seed, part) draws one part's arguments, and reference() takes and returns one part's arrays. A program takes and returns all parts, laid end to end along the dimension named above; each array names one. Nothing has to cross between parts.
Inputs may be any that keep to these rules, and one draw needn't show every extreme that they name: The 8 blocks of selected[t, g] are different and include block t // 64 and block 0. Over the 128 tokens of one device of ctx, the blocks named for one group that lie on other devices number exactly 7, at most one of each other device; block 0 is among them for every device but the first.
All inputs are finite; a program needn't handle non-finite values.
Results may differ from the reference program's by a relative error of at most 0.0075.
Values may be sent and summed in bfloat16 or wider, within the bound.
No kernel may reach another device: no remote copies, remote signals or barrier semaphores. Data moves between devices by JAX's collectives and lax.ppermute only.
A program may use at most 128 MiB of HBM per device.

```python
import math
import jax
import jax.numpy as jnp
from jax import lax

HEADS = 32
KVG = 2
DH = 128
BLK = 64
SEL = 8
TOK_DEV = 128
BPD = 2
OTHERS = 6
FG = 7
POOLB = 9
SEQ = 8192
N_CTX = 64


def choose_blocks(key):
    base = jax.random.fold_in(key, 11)
    first, second, third, fourth = jax.random.split(base, 4)
    requesters = jnp.arange(N_CTX).astype(jnp.int32)[:, None]
    owner_ids = jnp.arange(N_CTX).astype(jnp.int32)[None, :]
    noise = jax.random.randint(first, (N_CTX, N_CTX), 0, 1 << 20)
    ranking = noise * N_CTX + owner_ids + jnp.where(owner_ids < requesters, 1 << 27, 0)
    ranking = jnp.where((owner_ids == requesters) | (owner_ids == 0), -1, ranking)
    unused, ranked = lax.top_k(ranking, FG)
    with_sink = jnp.concatenate([jnp.zeros((N_CTX, 1), jnp.int32), ranked[:, :OTHERS]], axis=1)
    owner_list = jnp.where(requesters > 0, with_sink, ranked).astype(jnp.int32)
    local_ids = jax.random.randint(second, (N_CTX, FG, KVG), 0, BPD)
    local_ids = jnp.where(owner_list[..., None] == 0, 0, local_ids)
    far_blocks = owner_list[..., None] * BPD + local_ids
    own_blocks = requesters * BPD + jnp.arange(BPD).astype(jnp.int32)[None, :]
    own_blocks = jnp.broadcast_to(own_blocks[:, :, None], (N_CTX, BPD, KVG))
    pool_ids = jnp.concatenate([own_blocks, far_blocks], axis=1).transpose(0, 2, 1)
    pool_tokens = jnp.repeat(pool_ids, TOK_DEV, axis=0)
    token_ids = jnp.arange(SEQ).astype(jnp.int32)
    slot_ids = jnp.arange(POOLB).astype(jnp.int32)
    needed = (pool_tokens == (token_ids // BLK)[:, None, None]) | (pool_tokens == 0)
    needed = needed | (slot_ids[None, None, :] == (token_ids % TOK_DEV % POOLB)[:, None, None])
    shuffle = jax.random.randint(third, (SEQ, KVG, POOLB), 0, 1 << 20)
    marks = shuffle * POOLB + slot_ids + jnp.where(needed, 1 << 26, 0)
    unused_top, picks = lax.top_k(marks, SEL)
    chosen = jnp.take_along_axis(pool_tokens, picks, axis=2)
    reorder = jax.random.randint(fourth, (SEQ, KVG, SEL), 0, 1 << 20) * SEL + jnp.arange(SEL).astype(jnp.int32)
    order = jnp.argsort(reorder, axis=2)
    return jnp.take_along_axis(chosen, order, axis=2).astype(jnp.int32)


def query_key_pair(key):
    base = jax.random.fold_in(key, 23)
    first, second = jax.random.split(base, 2)
    key_base = jnp.clip(jax.random.normal(first, (SEQ, KVG, DH), jnp.float32), -5.0, 5.0)
    key_vals = key_base
    query_vals = jnp.clip(2.0 * jax.random.normal(second, (SEQ, HEADS, DH), jnp.float32), -12.0, 12.0)
    return (query_vals, key_vals)


def draw_queries(key, part):
    query_vals, key_vals = query_key_pair(key)
    return query_vals.astype(jnp.bfloat16)


def draw_keys(key, part):
    query_vals, key_vals = query_key_pair(key)
    return key_vals.astype(jnp.bfloat16)


def draw_selected(key, part):
    return choose_blocks(key)


def block_levels(stream_key, shape, cuts, low, largest):
    level, own = 1.0, jax.random.fold_in(stream_key, 6)
    for position, blocks in cuts:
        draws = jnp.exp(jax.random.uniform(jax.random.fold_in(own, position), (blocks,), jnp.float32, low / len(cuts), largest / len(cuts)))
        level = level * jnp.repeat(draws, shape[position] // blocks).reshape([-1 if axis == position else 1 for axis in range(len(shape))])
    return level


def normal_values(stream_key, dims, deviation, reach, cuts=(), held_as=jnp.bfloat16):
    entries = jax.random.normal(stream_key, dims, jnp.float32) * deviation
    if len(cuts) > 0:
        entries = block_levels(stream_key, dims, cuts, -0.22, 0.18) * entries
    return jnp.clip(entries, min=-reach, max=reach).astype(held_as)


def setup_inputs(seed: int = 0, part: int = 0) -> dict:
    splits = jax.random.split(jax.random.key(seed), 6)
    own_keys = jax.random.split(jax.random.fold_in(splits[5], part), 6)
    return {
        "queries": draw_queries(jax.random.fold_in(jax.random.fold_in(splits[5], part), 71), part),
        "keys": draw_keys(jax.random.fold_in(jax.random.fold_in(splits[5], part), 71), part),
        "values": normal_values(own_keys[2], (SEQ, KVG, DH), 1.0, 6.0, ((0, 64),)),
        "grad_out": normal_values(own_keys[3], (SEQ, HEADS, DH), 1.0, 6.0, ((0, 64),)),
        "selected": draw_selected(jax.random.fold_in(jax.random.fold_in(splits[5], part), 71), part),
    }


def reference(queries, keys, values, grad_out, selected):
    seq_len, head_count, head_dim = queries.shape
    groups = keys.shape[1]
    per_group = head_count // groups
    scaling = 1.0 / math.sqrt(head_dim)
    tile_rows = min(seq_len, 64)
    step_count = seq_len // tile_rows
    keys_by_group = keys.transpose(1, 0, 2)
    values_by_group = values.transpose(1, 0, 2)
    group_ids = jnp.arange(groups).astype(jnp.int32)[None, :, None]
    offsets = jnp.arange(BLK).astype(jnp.int32)

    def visit(carry, inputs):
        key_acc, value_acc = carry
        query_blk, upstream, chosen, first = inputs
        positions = (chosen[..., None] * BLK + offsets).reshape(tile_rows, groups, -1).astype(jnp.int32)
        key_rows = keys_by_group[group_ids, positions].astype(jnp.float32)
        value_rows = values_by_group[group_ids, positions].astype(jnp.float32)
        query_f = query_blk.astype(jnp.float32).reshape(tile_rows, groups, per_group, head_dim)
        upstream_f = upstream.astype(jnp.float32).reshape(tile_rows, groups, per_group, head_dim)
        scores = jnp.einsum('tghd,tgld->tghl', query_f, key_rows) * scaling
        query_pos = first + jnp.arange(tile_rows).astype(jnp.int32)
        allowed = positions <= query_pos[:, None, None]
        scores = jnp.where(allowed[:, :, None, :], scores, -jnp.inf)
        row_peak = lax.optimization_barrier(jnp.max(scores, axis=-1, keepdims=True))
        weights = jnp.exp(scores - row_peak)
        weights = weights / lax.optimization_barrier(jnp.sum(weights, axis=-1, keepdims=True))
        slope_grad = jnp.einsum('tghd,tgld->tghl', upstream_f, value_rows)
        row_inner = lax.optimization_barrier(jnp.sum(weights * slope_grad, axis=-1, keepdims=True))
        dscore = lax.optimization_barrier((weights * (slope_grad - row_inner) * scaling).astype(jnp.bfloat16))
        weights_low = lax.optimization_barrier(weights.astype(jnp.bfloat16))
        dscore_f = dscore.astype(jnp.float32)
        weights_f = weights_low.astype(jnp.float32)
        dquery = jnp.einsum('tghl,tgld->tghd', dscore_f, key_rows).astype(jnp.bfloat16)
        key_part = jnp.einsum('tghl,tghd->tgld', dscore_f, query_f)
        value_part = jnp.einsum('tghl,tghd->tgld', weights_f, upstream_f)
        key_acc = key_acc.at[group_ids, positions].add(key_part)
        value_acc = value_acc.at[group_ids, positions].add(value_part)
        return ((key_acc, value_acc), dquery.reshape(tile_rows, head_count, head_dim))
    inputs = (queries.reshape(step_count, tile_rows, head_count, head_dim), grad_out.reshape(step_count, tile_rows, head_count, head_dim), selected.reshape(step_count, tile_rows, groups, -1), (jnp.arange(step_count) * tile_rows).astype(jnp.int32))
    zeros_init = jnp.zeros((groups, seq_len, head_dim), jnp.float32)
    (key_acc, value_acc), dquery = lax.scan(visit, (zeros_init, zeros_init), inputs)
    dquery = dquery.reshape(seq_len, head_count, head_dim)
    key_grad = key_acc.transpose(1, 0, 2).astype(jnp.bfloat16)
    value_grad = value_acc.transpose(1, 0, 2).astype(jnp.bfloat16)
    return (dquery, key_grad, value_grad)
```

```python
import functools
import math

import jax
import jax.numpy as jnp
from jax import lax
from jax.experimental import pallas as pl
from jax.experimental.pallas import tpu as pltpu
from jax.sharding import PartitionSpec as P

BLK = 64
HEADS_PER_STEP = 2


def attend_kernel(
    place_ref,
    twin_ref,
    kv_ref,
    hide_ref,
    q0_ref,
    q1_ref,
    g0_ref,
    g1_ref,
    part_ref,
    dq0_ref,
    dq1_ref,
    keys_buf,
    keys_t_buf,
    values_buf,
    key_acc,
    value_acc,
    *,
    pool,
    scaling,
):
    step = pl.program_id(0)
    last = pl.num_programs(0) - 1

    @pl.when(step == 0)
    def _():
        for sub in range(2):
            for slot in range(pool):
                chunk = place_ref[sub, slot] // 2
                block = place_ref[sub, slot] % 2
                rows = pl.ds(slot * BLK, BLK)
                keys_buf[sub, rows, :] = kv_ref[chunk, 0, block]
                values_buf[sub, rows, :] = kv_ref[chunk, 1, block]
            keys_t_buf[sub] = keys_buf[sub].T
        key_acc[...] = jnp.zeros_like(key_acc)
        value_acc[...] = jnp.zeros_like(value_acc)
        part_ref[...] = jnp.zeros_like(part_ref)

    contract_last = (((1,), (1,)), ((), ()))
    for sub, (q_ref, g_ref, dq_ref) in enumerate(
        ((q0_ref, g0_ref, dq0_ref), (q1_ref, g1_ref, dq1_ref))
    ):
        heads, tokens, head_dim = q_ref.shape
        query_rows = q_ref[...].reshape(heads * tokens, head_dim)
        upstream_rows = g_ref[...].reshape(heads * tokens, head_dim)
        hide = jnp.concatenate([hide_ref[sub]] * heads, axis=1)
        scores = lax.dot_general(
            keys_buf[sub], query_rows, contract_last, preferred_element_type=jnp.float32
        )
        scores = scores * (scaling * math.log2(math.e)) + hide
        peak = jnp.max(scores, axis=0, keepdims=True)
        weights = jnp.exp2(scores - peak)
        total = jnp.sum(weights, axis=0, keepdims=True)
        slope = lax.dot_general(
            values_buf[sub], upstream_rows, contract_last, preferred_element_type=jnp.float32
        )
        share = 1.0 / total
        inner = jnp.sum(weights * slope, axis=0, keepdims=True) * share
        weights = weights * share
        dscore = (weights * (slope - inner) * scaling).astype(jnp.bfloat16)
        weights_low = weights.astype(jnp.bfloat16)
        dquery_t = jnp.dot(keys_t_buf[sub], dscore, preferred_element_type=jnp.float32)
        dq_ref[...] = dquery_t.T.astype(jnp.bfloat16).reshape(heads, tokens, head_dim)
        key_acc[sub] += jnp.dot(dscore, query_rows, preferred_element_type=jnp.float32)
        value_acc[sub] += jnp.dot(weights_low, upstream_rows, preferred_element_type=jnp.float32)

    @pl.when(step == last)
    def _():
        for kind, acc in enumerate((key_acc, value_acc)):
            for slot in range(pool):
                chunk = place_ref[0, slot] // 2
                block = place_ref[0, slot] % 2
                rows = pl.ds(slot * BLK, BLK)
                part_ref[chunk, kind, block] = acc[0, rows, :].astype(jnp.bfloat16)
            for slot in range(pool):
                chunk = place_ref[1, slot] // 2
                block = place_ref[1, slot] % 2
                twin = twin_ref[slot]
                rows = pl.ds(slot * BLK, BLK)
                twin_rows = pl.ds(pl.multiple_of(jnp.maximum(twin, 0) * BLK, BLK), BLK)
                shared = jnp.where(twin >= 0, acc[0, twin_rows, :], 0.0)
                part_ref[chunk, kind, block] = (acc[1, rows, :] + shared).astype(jnp.bfloat16)


def attend(place, twin, kv, hide, q0, q1, g0, g1, pool):
    heads, tokens, head_dim = q0.shape
    keys = pool * BLK
    per_step = HEADS_PER_STEP
    whole = lambda shape: pl.BlockSpec(shape, lambda i, *_: (0,) * len(shape))
    by_head = pl.BlockSpec((per_step, tokens, head_dim), lambda i, *_: (i, 0, 0))
    grid_spec = pltpu.PrefetchScalarGridSpec(
        num_scalar_prefetch=2,
        grid=(heads // per_step,),
        in_specs=[whole(kv.shape), whole(hide.shape), by_head, by_head, by_head, by_head],
        out_specs=[whole(kv.shape), by_head, by_head],
        scratch_shapes=[
            pltpu.VMEM((2, keys, head_dim), jnp.bfloat16),
            pltpu.VMEM((2, head_dim, keys), jnp.bfloat16),
            pltpu.VMEM((2, keys, head_dim), jnp.bfloat16),
            pltpu.VMEM((2, keys, head_dim), jnp.float32),
            pltpu.VMEM((2, keys, head_dim), jnp.float32),
        ],
    )
    return pl.pallas_call(
        functools.partial(attend_kernel, pool=pool, scaling=1.0 / math.sqrt(head_dim)),
        grid_spec=grid_spec,
        out_shape=[
            jax.ShapeDtypeStruct(kv.shape, jnp.bfloat16),
            jax.ShapeDtypeStruct(q0.shape, jnp.bfloat16),
            jax.ShapeDtypeStruct(q0.shape, jnp.bfloat16),
        ],
        compiler_params=pltpu.CompilerParams(dimension_semantics=("arbitrary",)),
        cost_estimate=pl.CostEstimate(
            flops=2 * 5 * 2 * heads * tokens * keys * head_dim,
            bytes_accessed=16 * 2**20,
            transcendentals=2 * heads * tokens * keys,
        ),
    )(place, twin, kv, hide, q0, q1, g0, g1)


def choose_pool(chosen, device, core, chip, owners, own_blocks, fetched):
    tokens = chosen.shape[0]
    chips = owners // 2
    ids = jnp.arange(owners * own_blocks, dtype=jnp.int32)
    named = jnp.any(chosen.reshape(-1, 1) == ids[None, :], axis=0)
    far = named & (ids // own_blocks != device)
    rank = jnp.sum(jnp.where(far[:, None] & (ids[:, None] < ids[None, :]), 1, 0), axis=0)
    picker = far[None, :] & (rank[None, :] == jnp.arange(fetched, dtype=jnp.int32)[:, None])
    far_blocks = jnp.sum(jnp.where(picker, ids[None, :], 0), axis=1)
    blocks = jnp.concatenate([device * own_blocks + jnp.arange(own_blocks, dtype=jnp.int32), far_blocks])
    owner = blocks // own_blocks
    half = (owner % 2) ^ core
    away = (chip - owner // 2) % chips
    half_way = chips // 2
    chunk = jnp.where(
        away == 0,
        half,
        jnp.where(away <= half_way, 4 * away - 2 + half, 4 * (chips - away) + half),
    )
    place = chunk * own_blocks + blocks % own_blocks
    picked = jnp.any(chosen[None, :, :] == blocks[:, None, None], axis=2)
    key_pos = blocks[:, None] * BLK + jnp.arange(BLK, dtype=jnp.int32)[None, :]
    query_pos = device * tokens + jnp.arange(tokens, dtype=jnp.int32)
    visible = picked[:, None, :] & (key_pos[:, :, None] <= query_pos[None, None, :])
    hide = jnp.where(visible, 0.0, -jnp.inf).astype(jnp.float32)
    return place, hide.reshape(-1, tokens)


def local(queries, keys, values, grad_out, selected):
    tokens, head_count, head_dim = queries.shape
    groups = keys.shape[1]
    per_group = head_count // groups
    own_blocks = tokens // BLK
    owners = lax.axis_size("ctx")
    chips = owners // 2
    half_way = chips // 2
    fetched = min(owners - 2, max(selected.shape[2] - own_blocks, 4)) + 1
    pool = own_blocks + fetched
    device = lax.axis_index("ctx").astype(jnp.int32)
    chip = device // 2
    core = device % 2
    first = core == 0

    def move(x, hops, change=False):
        pairs = []
        for src in range(owners):
            dst_core = (src % 2) ^ int(change)
            pairs.append((src, 2 * ((src // 2 + hops) % chips) + dst_core))
        return lax.ppermute(x, "ctx", pairs)

    def mine_other(zero, one):
        return jnp.where(first, zero, one), jnp.where(first, one, zero)

    kv0 = jnp.stack([keys[:, 0], values[:, 0]])
    kv1 = jnp.stack([keys[:, 1], values[:, 1]])
    kv_mine, kv_other = mine_other(kv0, kv1)

    up_same, up_cross = move(kv_mine, 1), move(kv_other, 1, True)
    down_same, down_cross = move(kv_mine, -1), move(kv_other, -1, True)
    kv_partner = move(kv_other, 0, True)
    chunks = [kv_mine, kv_partner]
    for hop in range(1, half_way + 1):
        chunks += [up_same, up_cross]
        if hop < half_way:
            chunks += [down_same, down_cross]
            up_same, up_cross = move(up_same, 1), move(up_cross, 1)
        if hop < half_way - 1:
            down_same, down_cross = move(down_same, -1), move(down_cross, -1)
    gathered = jnp.stack(chunks).reshape(2 * chips, 2, own_blocks, BLK, head_dim)

    sel_mine, sel_other = mine_other(selected[:, 0], selected[:, 1])
    sel_partner = move(sel_other, 0, True)
    place0, hide0 = choose_pool(sel_mine, device, core, chip, owners, own_blocks, fetched)
    place1, hide1 = choose_pool(sel_partner, device ^ 1, core, chip, owners, own_blocks, fetched)
    same = place1[:, None] == place0[None, :]
    twin = jnp.max(jnp.where(same, jnp.arange(pool, dtype=jnp.int32)[None, :], -1), axis=1)
    place = jnp.stack([place0, place1])
    hide = jnp.stack([hide0, hide1])

    def split_heads(x):
        return mine_other(x[:, :per_group], x[:, per_group:])

    def heads_first(x):
        return x.transpose(1, 0, 2)

    q_mine, q_other = split_heads(queries)
    g_mine, g_other = split_heads(grad_out)
    q_partner = move(q_other, 0, True)
    g_partner = move(g_other, 0, True)

    part, dq_mine, dq_partner = attend(
        place,
        twin,
        gathered,
        hide,
        heads_first(q_mine),
        heads_first(q_partner),
        heads_first(g_mine),
        heads_first(g_partner),
        pool,
    )
    part = part.reshape(2 * chips, 2, tokens, head_dim)
    f32 = jnp.float32

    def piece(index):
        return part[2 * index : 2 * index + 2]

    down = piece(2 * half_way - 1)
    up = piece(2 * half_way - 2)
    for hop in range(half_way - 1, 0, -1):
        down = move(down, -1)
        down = (down.astype(f32) + piece(2 * hop - 1).astype(f32)).astype(jnp.bfloat16)
        if hop < half_way - 1:
            up = move(up, 1)
            up = (up.astype(f32) + piece(2 * hop).astype(f32)).astype(jnp.bfloat16)
    grad_same = (
        part[0].astype(f32) + move(down[0], -1).astype(f32) + move(up[0], 1).astype(f32)
    )
    grad_cross = (
        move(part[1], 0, True).astype(f32)
        + move(down[1], -1, True).astype(f32)
        + move(up[1], 1, True).astype(f32)
    )
    zero, one = mine_other(grad_same, grad_cross)
    key_grad = jnp.stack([zero[0], one[0]], axis=1).astype(jnp.bfloat16)
    value_grad = jnp.stack([zero[1], one[1]], axis=1).astype(jnp.bfloat16)

    dq_other = move(dq_partner, 0, True)
    dq_zero, dq_one = mine_other(dq_mine, dq_other)
    dquery = jnp.concatenate([dq_zero, dq_one], axis=0).transpose(1, 0, 2)
    return (dquery, key_grad, value_grad)


def solution(mesh):
    spec = P(("rep", "ctx"), None, None)
    return jax.shard_map(
        local,
        mesh=mesh,
        in_specs=(spec,) * 5,
        out_specs=(spec,) * 3,
        check_vma=False,
    )
```

```python
import functools
import math

import jax
import jax.numpy as jnp
from jax import lax
from jax.experimental import pallas as pl
from jax.experimental.pallas import tpu as pltpu
from jax.sharding import PartitionSpec as P

BLK = 64
HEADS_PER_STEP = 2


def attend_kernel(*refs, chunks, pool, scaling):
    place0_ref, place1_ref, twin_ref, *refs = refs
    kv_refs, refs = refs[:chunks], refs[chunks:]
    hide0_ref, hide1_ref, q0_ref, q1_ref, g0_ref, g1_ref, *refs = refs
    part_refs, refs = refs[:chunks], refs[chunks:]
    dq0_ref, dq1_ref, kv_buf, part_buf, sems, *refs = refs
    keys_buf, keys_t_buf, values_buf, key_acc, value_acc = refs
    step = pl.program_id(0)
    last = pl.num_programs(0) - 1

    def spot(place_ref, slot):
        at = place_ref[slot]
        return at // 4, (at // 2) % 2, at % 2

    @pl.when(step == 0)
    def _():
        loads = [
            pltpu.make_async_copy(ref, kv_buf.at[i], sems.at[i]) for i, ref in enumerate(kv_refs)
        ]
        for load in loads:
            load.start()
        key_acc[...] = jnp.zeros_like(key_acc)
        value_acc[...] = jnp.zeros_like(value_acc)
        part_buf[...] = jnp.zeros_like(part_buf)
        for load in loads:
            load.wait()
        for sub, place_ref in enumerate((place0_ref, place1_ref)):
            for slot in range(pool):
                chunk, half, block = spot(place_ref, slot)
                rows = pl.ds(slot * BLK, BLK)
                keys_buf[sub, rows, :] = kv_buf[chunk, half, 0, block]
                values_buf[sub, rows, :] = kv_buf[chunk, half, 1, block]
            keys_t_buf[sub] = keys_buf[sub].T

    contract_last = (((1,), (1,)), ((), ()))
    for sub, (q_ref, g_ref, hide_ref, dq_ref) in enumerate(
        ((q0_ref, g0_ref, hide0_ref, dq0_ref), (q1_ref, g1_ref, hide1_ref, dq1_ref))
    ):
        heads, tokens, head_dim = q_ref.shape
        query_rows = q_ref[...].reshape(heads * tokens, head_dim)
        upstream_rows = g_ref[...].reshape(heads * tokens, head_dim)
        hide = jnp.concatenate([hide_ref[...]] * heads, axis=1)
        scores = lax.dot_general(
            keys_buf[sub], query_rows, contract_last, preferred_element_type=jnp.float32
        )
        scores = scores * (scaling * math.log2(math.e)) + hide
        peak = jnp.max(scores, axis=0, keepdims=True)
        weights = jnp.exp2(scores - peak)
        total = jnp.sum(weights, axis=0, keepdims=True)
        slope = lax.dot_general(
            values_buf[sub], upstream_rows, contract_last, preferred_element_type=jnp.float32
        )
        share = 1.0 / total
        inner = jnp.sum(weights * slope, axis=0, keepdims=True) * share
        weights_low = (weights * share).astype(jnp.bfloat16)
        dscore = (weights * ((slope - inner) * (share * scaling))).astype(jnp.bfloat16)
        dquery_t = jnp.dot(keys_t_buf[sub], dscore, preferred_element_type=jnp.float32)
        dq_ref[...] = dquery_t.T.astype(jnp.bfloat16).reshape(heads, tokens, head_dim)
        key_acc[sub] += jnp.dot(dscore, query_rows, preferred_element_type=jnp.float32)
        value_acc[sub] += jnp.dot(weights_low, upstream_rows, preferred_element_type=jnp.float32)

    @pl.when(step == last)
    def _():
        for kind, acc in enumerate((key_acc, value_acc)):
            for slot in range(pool):
                chunk, half, block = spot(place0_ref, slot)
                rows = pl.ds(slot * BLK, BLK)
                part_buf[chunk, half, kind, block] = acc[0, rows, :].astype(jnp.bfloat16)
            for slot in range(pool):
                chunk, half, block = spot(place1_ref, slot)
                twin = twin_ref[slot]
                rows = pl.ds(slot * BLK, BLK)
                twin_rows = pl.ds(pl.multiple_of(jnp.maximum(twin, 0) * BLK, BLK), BLK)
                shared = jnp.where(twin >= 0, acc[0, twin_rows, :], 0.0)
                part_buf[chunk, half, kind, block] = (acc[1, rows, :] + shared).astype(jnp.bfloat16)
        stores = [
            pltpu.make_async_copy(part_buf.at[i], ref, sems.at[i]) for i, ref in enumerate(part_refs)
        ]
        for store in stores:
            store.start()
        for store in stores:
            store.wait()


def attend(place0, place1, twin, kv, hide0, hide1, q0, q1, g0, g1, pool):
    heads, tokens, head_dim = q0.shape
    keys = pool * BLK
    chunks = len(kv)
    per_step = HEADS_PER_STEP
    anywhere = [pl.BlockSpec(memory_space=pl.ANY)] * chunks
    whole = pl.BlockSpec(hide0.shape, lambda i, *_: (0, 0))
    by_head = pl.BlockSpec((per_step, tokens, head_dim), lambda i, *_: (i, 0, 0))
    grid_spec = pltpu.PrefetchScalarGridSpec(
        num_scalar_prefetch=3,
        grid=(heads // per_step,),
        in_specs=[*anywhere, whole, whole, by_head, by_head, by_head, by_head],
        out_specs=[*anywhere, by_head, by_head],
        scratch_shapes=[
            pltpu.VMEM((chunks, *kv[0].shape), jnp.bfloat16),
            pltpu.VMEM((chunks, *kv[0].shape), jnp.bfloat16),
            pltpu.SemaphoreType.DMA((chunks,)),
            pltpu.VMEM((2, keys, head_dim), jnp.bfloat16),
            pltpu.VMEM((2, head_dim, keys), jnp.bfloat16),
            pltpu.VMEM((2, keys, head_dim), jnp.bfloat16),
            pltpu.VMEM((2, keys, head_dim), jnp.float32),
            pltpu.VMEM((2, keys, head_dim), jnp.float32),
        ],
    )
    *part, dq0, dq1 = pl.pallas_call(
        functools.partial(
            attend_kernel, chunks=chunks, pool=pool, scaling=1.0 / math.sqrt(head_dim)
        ),
        grid_spec=grid_spec,
        out_shape=[
            *[jax.ShapeDtypeStruct(x.shape, jnp.bfloat16) for x in kv],
            jax.ShapeDtypeStruct(q0.shape, jnp.bfloat16),
            jax.ShapeDtypeStruct(q0.shape, jnp.bfloat16),
        ],
        compiler_params=pltpu.CompilerParams(dimension_semantics=("arbitrary",)),
        cost_estimate=pl.CostEstimate(
            flops=2 * 5 * 2 * heads * tokens * keys * head_dim,
            bytes_accessed=16 * 2**20,
            transcendentals=2 * heads * tokens * keys,
        ),
    )(place0, place1, twin, *kv, hide0, hide1, q0, q1, g0, g1)
    return part, dq0, dq1


def choose_pool(chosen, device, core, chip, owners, own_blocks, fetched):
    tokens = chosen.shape[0]
    chips = owners // 2
    ids = jnp.arange(owners * own_blocks, dtype=jnp.int32)
    named = jnp.any(chosen.reshape(-1, 1) == ids[None, :], axis=0)
    far = named & (ids // own_blocks != device)
    rank = jnp.sum(jnp.where(far[:, None] & (ids[:, None] < ids[None, :]), 1, 0), axis=0)
    picker = far[None, :] & (rank[None, :] == jnp.arange(fetched, dtype=jnp.int32)[:, None])
    far_blocks = jnp.sum(jnp.where(picker, ids[None, :], 0), axis=1)
    blocks = jnp.concatenate([device * own_blocks + jnp.arange(own_blocks, dtype=jnp.int32), far_blocks])
    owner = blocks // own_blocks
    half = (owner % 2) ^ core
    away = (chip - owner // 2) % chips
    half_way = chips // 2
    chunk = jnp.where(away <= half_way, away, half_way + chips - away)
    place = (2 * chunk + half) * own_blocks + blocks % own_blocks
    picked = jnp.any(chosen[None, :, :] == blocks[:, None, None], axis=2)
    key_pos = blocks[:, None] * BLK + jnp.arange(BLK, dtype=jnp.int32)[None, :]
    query_pos = device * tokens + jnp.arange(tokens, dtype=jnp.int32)
    visible = picked[:, None, :] & (key_pos[:, :, None] <= query_pos[None, None, :])
    hide = jnp.where(visible, 0.0, -jnp.inf).astype(jnp.float32)
    return place, hide.reshape(-1, tokens)


def local(queries, keys, values, grad_out, selected):
    tokens, head_count, head_dim = queries.shape
    groups = keys.shape[1]
    per_group = head_count // groups
    own_blocks = tokens // BLK
    owners = lax.axis_size("ctx")
    chips = owners // 2
    half_way = chips // 2
    fetched = min(owners - 2, max(selected.shape[2] - own_blocks, 4)) + 1
    pool = own_blocks + fetched
    device = lax.axis_index("ctx").astype(jnp.int32)
    chip = device // 2
    core = device % 2
    first = core == 0

    def move(x, hops, change=False):
        pairs = []
        for src in range(owners):
            dst_core = (src % 2) ^ int(change)
            pairs.append((src, 2 * ((src // 2 + hops) % chips) + dst_core))
        return lax.ppermute(x, "ctx", pairs)

    def mine_other(zero, one):
        return jnp.where(first, zero, one), jnp.where(first, one, zero)

    kv0 = jnp.stack([keys[:, 0], values[:, 0]])
    kv1 = jnp.stack([keys[:, 1], values[:, 1]])
    kv_mine, kv_other = mine_other(kv0, kv1)

    kv_partner = move(kv_other, 0, True)
    ups = [jnp.stack([move(kv_mine, 1), move(kv_other, 1, True)])]
    downs = [jnp.stack([move(kv_mine, -1), move(kv_other, -1, True)])]
    for hop in range(1, half_way):
        ups.append(move(ups[-1], 1))
        if hop < half_way - 1:
            downs.append(move(downs[-1], -1))
    gathered = [jnp.stack([kv_mine, kv_partner]), *ups, *downs]
    gathered = [x.reshape(2, 2, own_blocks, BLK, head_dim) for x in gathered]

    def held(x, hop):
        return lax.optimization_barrier((x, ups[hop - 1]))[0]

    chosen = held(selected, 2)
    sel_mine, sel_other = mine_other(chosen[:, 0], chosen[:, 1])
    sel_partner = move(sel_other, 0, True)
    place0, hide0 = choose_pool(held(sel_mine, 7), device, core, chip, owners, own_blocks, fetched)
    place1, hide1 = choose_pool(held(sel_partner, 9), device ^ 1, core, chip, owners, own_blocks, fetched)
    same = place1[:, None] == place0[None, :]
    twin = jnp.max(jnp.where(same, jnp.arange(pool, dtype=jnp.int32)[None, :], -1), axis=1)

    def split_heads(x):
        return mine_other(x[:, :per_group], x[:, per_group:])

    def heads_first(x):
        return x.transpose(1, 0, 2)

    q_mine, q_other = split_heads(held(queries, 3))
    g_mine, g_other = split_heads(held(grad_out, 5))
    q_partner = move(q_other, 0, True)
    g_partner = move(g_other, 0, True)

    part, dq_mine, dq_partner = attend(
        place0,
        place1,
        twin,
        gathered,
        hide0,
        hide1,
        heads_first(q_mine),
        heads_first(q_partner),
        heads_first(g_mine),
        heads_first(g_partner),
        pool,
    )
    own, *part = [x.reshape(2, 2, tokens, head_dim) for x in part]
    f32 = jnp.float32

    down = part[half_way - 1]
    up = part[-1]
    for hop in range(half_way - 1, 0, -1):
        down = move(down, -1)
        down = (down.astype(f32) + part[hop - 1].astype(f32)).astype(jnp.bfloat16)
        if hop < half_way - 1:
            up = move(up, 1)
            up = (up.astype(f32) + part[half_way + hop - 1].astype(f32)).astype(jnp.bfloat16)
    grad_same = own[0].astype(f32) + move(down[0], -1).astype(f32) + move(up[0], 1).astype(f32)
    grad_cross = (
        move(own[1], 0, True).astype(f32)
        + move(down[1], -1, True).astype(f32)
        + move(up[1], 1, True).astype(f32)
    )
    zero, one = mine_other(grad_same, grad_cross)
    key_grad = jnp.stack([zero[0], one[0]], axis=1).astype(jnp.bfloat16)
    value_grad = jnp.stack([zero[1], one[1]], axis=1).astype(jnp.bfloat16)

    dq_other = move(dq_partner, 0, True)
    dq_zero, dq_one = mine_other(dq_mine, dq_other)
    dquery = jnp.concatenate([dq_zero, dq_one], axis=0).transpose(1, 0, 2)
    return (dquery, key_grad, value_grad)


def solution(mesh):
    spec = P(("rep", "ctx"), None, None)
    return jax.shard_map(
        local,
        mesh=mesh,
        in_specs=(spec,) * 5,
        out_specs=(spec,) * 3,
        check_vma=False,
    )
```

```python
import functools
import math

import jax
import jax.numpy as jnp
from jax import lax
from jax.experimental import pallas as pl
from jax.experimental.pallas import tpu as pltpu
from jax.sharding import PartitionSpec as P

BLK = 64
VMEM_LIMIT = 44 * 2**20


def attend_kernel(*refs, chunks, pool, scaling):
    place0_ref, place1_ref, twin_ref, needed_ref, *refs = refs
    kv_refs, refs = refs[:chunks], refs[chunks:]
    hide0_ref, hide1_ref, q0_ref, q1_ref, g0_ref, g1_ref, *refs = refs
    part_refs, refs = refs[:chunks], refs[chunks:]
    dq0_ref, dq1_ref, kv_buf, part_buf, sems, *refs = refs
    keys_buf, keys_t_buf, values_buf, key_acc, value_acc = refs

    def spot(place_ref, slot):
        at = place_ref[slot]
        return at // 2, at % 2

    loads = [pltpu.make_async_copy(ref, kv_buf.at[i], sems.at[i]) for i, ref in enumerate(kv_refs)]
    for i, load in enumerate(loads):
        pl.when(needed_ref[i] > 0)(load.start)
    part_buf[...] = jnp.zeros_like(part_buf)
    for i, load in enumerate(loads):
        pl.when(needed_ref[i] > 0)(load.wait)
    contract_last = (((1,), (1,)), ((), ()))
    for sub, (place_ref, q_ref, g_ref, hide_ref, dq_ref) in enumerate(
        (
            (place0_ref, q0_ref, g0_ref, hide0_ref, dq0_ref),
            (place1_ref, q1_ref, g1_ref, hide1_ref, dq1_ref),
        )
    ):
        for slot in range(pool):
            chunk, block = spot(place_ref, slot)
            rows = pl.ds(slot * BLK, BLK)
            keys_buf[sub, rows, :] = kv_buf[chunk, 0, block]
            values_buf[sub, rows, :] = kv_buf[chunk, 1, block]
        keys_t_buf[sub] = keys_buf[sub].T
        heads, tokens, head_dim = q_ref.shape
        query_rows = q_ref[...].reshape(heads * tokens, head_dim)
        upstream_rows = g_ref[...].reshape(heads * tokens, head_dim)
        hide = jnp.concatenate([hide_ref[...]] * heads, axis=1)
        scores = lax.dot_general(
            keys_buf[sub], query_rows, contract_last, preferred_element_type=jnp.float32
        )
        scores = scores * (scaling * math.log2(math.e)) + hide
        peak = jnp.max(scores, axis=0, keepdims=True)
        weights = jnp.exp2(scores - peak)
        total = jnp.sum(weights, axis=0, keepdims=True)
        slope = lax.dot_general(
            values_buf[sub], upstream_rows, contract_last, preferred_element_type=jnp.float32
        )
        share = 1.0 / total
        inner = jnp.sum(weights * slope, axis=0, keepdims=True) * share
        weights_low = (weights * share).astype(jnp.bfloat16)
        dscore = (weights * ((slope - inner) * (share * scaling))).astype(jnp.bfloat16)
        dquery_t = jnp.dot(keys_t_buf[sub], dscore, preferred_element_type=jnp.float32)
        dq_ref[...] = dquery_t.T.astype(jnp.bfloat16).reshape(heads, tokens, head_dim)
        key_acc[sub] = jnp.dot(dscore, query_rows, preferred_element_type=jnp.float32)
        value_acc[sub] = jnp.dot(weights_low, upstream_rows, preferred_element_type=jnp.float32)

    for kind, acc in enumerate((key_acc, value_acc)):
        for slot in range(pool):
            chunk, block = spot(place0_ref, slot)
            rows = pl.ds(slot * BLK, BLK)
            part_buf[chunk, kind, block] = acc[0, rows, :].astype(jnp.bfloat16)
        for slot in range(pool):
            chunk, block = spot(place1_ref, slot)
            twin = twin_ref[slot]
            rows = pl.ds(slot * BLK, BLK)
            twin_rows = pl.ds(pl.multiple_of(jnp.maximum(twin, 0) * BLK, BLK), BLK)
            shared = jnp.where(twin >= 0, acc[0, twin_rows, :], 0.0)
            part_buf[chunk, kind, block] = (acc[1, rows, :] + shared).astype(jnp.bfloat16)
    for i, ref in enumerate(part_refs):
        ref[...] = part_buf[i]


def placed(shape):
    return pltpu.VMEM(shape, jnp.bfloat16)


def attend(place0, place1, twin, needed, kv, hide0, hide1, q0, q1, g0, g1, pool):
    heads, tokens, head_dim = q0.shape
    keys = pool * BLK
    chunks = len(kv)
    scalar = pl.BlockSpec(memory_space=pltpu.SMEM)
    whole = pl.BlockSpec(memory_space=pltpu.VMEM)
    wide = [
        pltpu.with_memory_space_constraint(x, pltpu.VMEM) for x in (hide0, hide1, q0, q1, g0, g1)
    ]
    far = [pltpu.with_memory_space_constraint(x, pltpu.HBM) for x in kv]
    *part, dq0, dq1 = pl.pallas_call(
        functools.partial(
            attend_kernel, chunks=chunks, pool=pool, scaling=1.0 / math.sqrt(head_dim)
        ),
        in_specs=[scalar] * 4 + [pl.BlockSpec(memory_space=pltpu.HBM)] * chunks + [whole] * len(wide),
        out_specs=[whole] * (chunks + 2),
        scratch_shapes=[
            pltpu.VMEM((chunks, *kv[0].shape), jnp.bfloat16),
            pltpu.VMEM((chunks, *kv[0].shape), jnp.bfloat16),
            pltpu.SemaphoreType.DMA((chunks,)),
            pltpu.VMEM((2, keys, head_dim), jnp.bfloat16),
            pltpu.VMEM((2, head_dim, keys), jnp.bfloat16),
            pltpu.VMEM((2, keys, head_dim), jnp.bfloat16),
            pltpu.VMEM((2, keys, head_dim), jnp.float32),
            pltpu.VMEM((2, keys, head_dim), jnp.float32),
        ],
        out_shape=[
            *[placed(x.shape) for x in kv],
            placed(q0.shape),
            placed(q0.shape),
        ],
        compiler_params=pltpu.CompilerParams(vmem_limit_bytes=VMEM_LIMIT),
        cost_estimate=pl.CostEstimate(
            flops=2 * 5 * 2 * heads * tokens * keys * head_dim,
            bytes_accessed=16 * 2**20,
            transcendentals=2 * heads * tokens * keys,
        ),
    )(place0, place1, twin, needed, *far, *wide)
    return part, dq0, dq1


def choose_pool(chosen, device, core, chip, owners, own_blocks, fetched):
    tokens = chosen.shape[0]
    chips = owners // 2
    ids = jnp.arange(owners * own_blocks, dtype=jnp.int32)
    named = jnp.any(chosen.reshape(-1, 1) == ids[None, :], axis=0)
    far = named & (ids // own_blocks != device)
    rank = jnp.sum(jnp.where(far[:, None] & (ids[:, None] < ids[None, :]), 1, 0), axis=0)
    picker = far[None, :] & (rank[None, :] == jnp.arange(fetched, dtype=jnp.int32)[:, None])
    far_blocks = jnp.sum(jnp.where(picker, ids[None, :], 0), axis=1)
    blocks = jnp.concatenate([device * own_blocks + jnp.arange(own_blocks, dtype=jnp.int32), far_blocks])
    owner = blocks // own_blocks
    half = (owner % 2) ^ core
    away = (chip - owner // 2) % chips
    half_way = chips // 2
    chunk = jnp.where(away <= half_way, away, half_way + chips - away)
    place = (2 * chunk + half) * own_blocks + blocks % own_blocks
    picked = jnp.any(chosen[None, :, :] == blocks[:, None, None], axis=2)
    key_pos = blocks[:, None] * BLK + jnp.arange(BLK, dtype=jnp.int32)[None, :]
    query_pos = device * tokens + jnp.arange(tokens, dtype=jnp.int32)
    visible = picked[:, None, :] & (key_pos[:, :, None] <= query_pos[None, None, :])
    hide = jnp.where(visible, 0.0, -jnp.inf).astype(jnp.float32)
    return place, hide.reshape(-1, tokens)


def local(queries, keys, values, grad_out, selected):
    tokens, head_count, head_dim = queries.shape
    groups = keys.shape[1]
    per_group = head_count // groups
    own_blocks = tokens // BLK
    owners = lax.axis_size("ctx")
    chips = owners // 2
    half_way = chips // 2
    fetched = min(owners - 2, max(selected.shape[2] - own_blocks, 4)) + 1
    pool = own_blocks + fetched
    device = lax.axis_index("ctx").astype(jnp.int32)
    chip = device // 2
    core = device % 2
    first = core == 0

    def move(x, hops, change=False):
        pairs = []
        for src in range(owners):
            dst_core = (src % 2) ^ int(change)
            pairs.append((src, 2 * ((src // 2 + hops) % chips) + dst_core))
        return lax.ppermute(x, "ctx", pairs)

    def mine_other(zero, one):
        return jnp.where(first, zero, one), jnp.where(first, one, zero)

    kv0 = jnp.stack([keys[:, 0], values[:, 0]])
    kv1 = jnp.stack([keys[:, 1], values[:, 1]])
    kv_mine, kv_other = mine_other(kv0, kv1)

    kv_partner = move(kv_other, 0, True)
    ups = [(move(kv_mine, 1), move(kv_other, 1, True))]
    downs = [(move(kv_mine, -1), move(kv_other, -1, True))]
    for hop in range(1, half_way):
        ups.append(tuple(move(x, 1) for x in ups[-1]))
        if hop < half_way - 1:
            downs.append(tuple(move(x, -1) for x in downs[-1]))
    gathered = [x for pair in ((kv_mine, kv_partner), *ups, *downs) for x in pair]
    gathered = [x.reshape(2, own_blocks, BLK, head_dim) for x in gathered]

    def held(x, hop):
        return lax.optimization_barrier((x, ups[hop - 1][0]))[0]

    chosen = held(selected, 2)
    sel_mine, sel_other = mine_other(chosen[:, 0], chosen[:, 1])
    sel_partner = move(sel_other, 0, True)
    place0, hide0 = choose_pool(held(sel_mine, 7), device, core, chip, owners, own_blocks, fetched)
    place1, hide1 = choose_pool(held(sel_partner, 9), device ^ 1, core, chip, owners, own_blocks, fetched)
    same = place1[:, None] == place0[None, :]
    twin = jnp.max(jnp.where(same, jnp.arange(pool, dtype=jnp.int32)[None, :], -1), axis=1)

    chunk_ids = jnp.arange(len(gathered), dtype=jnp.int32)[:, None]
    named = jnp.concatenate([place0, place1])[None, :] // own_blocks == chunk_ids
    needed = jnp.any(named, axis=1).astype(jnp.int32)

    def split_heads(x):
        return mine_other(x[:, :per_group], x[:, per_group:])

    def heads_first(x):
        return x.transpose(1, 0, 2)

    q_mine, q_other = split_heads(held(queries, 3))
    g_mine, g_other = split_heads(held(grad_out, 5))
    q_partner = move(q_other, 0, True)
    g_partner = move(g_other, 0, True)

    part, dq_mine, dq_partner = attend(
        place0,
        place1,
        twin,
        needed,
        gathered,
        hide0,
        hide1,
        heads_first(q_mine),
        heads_first(q_partner),
        heads_first(g_mine),
        heads_first(g_partner),
        pool,
    )
    part = [x.reshape(2, tokens, head_dim) for x in part]
    own, *part = zip(part[::2], part[1::2], strict=True)
    f32 = jnp.float32

    def add(x, y):
        return (x.astype(f32) + y.astype(f32)).astype(jnp.bfloat16)

    down = part[half_way - 1]
    up = part[-1]
    for hop in range(half_way - 1, 0, -1):
        down = [add(move(x, -1), y) for x, y in zip(down, part[hop - 1], strict=True)]
        if hop < half_way - 1:
            up = [add(move(x, 1), y) for x, y in zip(up, part[half_way + hop - 1], strict=True)]
    grad_same = own[0].astype(f32) + move(down[0], -1).astype(f32) + move(up[0], 1).astype(f32)
    grad_cross = (
        move(own[1], 0, True).astype(f32)
        + move(down[1], -1, True).astype(f32)
        + move(up[1], 1, True).astype(f32)
    )
    zero, one = mine_other(grad_same, grad_cross)
    key_grad = jnp.stack([zero[0], one[0]], axis=1).astype(jnp.bfloat16)
    value_grad = jnp.stack([zero[1], one[1]], axis=1).astype(jnp.bfloat16)

    dq_other = move(dq_partner, 0, True)
    dq_zero, dq_one = mine_other(dq_mine, dq_other)
    dquery = jnp.concatenate([dq_zero, dq_one], axis=0).transpose(1, 0, 2)
    return (dquery, key_grad, value_grad)


def solution(mesh):
    spec = P(("rep", "ctx"), None, None)
    return jax.shard_map(
        local,
        mesh=mesh,
        in_specs=(spec,) * 5,
        out_specs=(spec,) * 3,
        check_vma=False,
    )
```

```python
import functools
import math

import jax
import jax.numpy as jnp
from jax import lax
from jax.experimental import pallas as pl
from jax.experimental.pallas import tpu as pltpu
from jax.sharding import PartitionSpec as P

BLK = 64
VMEM_LIMIT = 44 * 2**20


def attend_kernel(*refs, chunks, pool, scaling):
    place0_ref, place1_ref, twin_ref, needed_ref, *refs = refs
    kv_refs, refs = refs[:chunks], refs[chunks:]
    hide0_ref, hide1_ref, q0_ref, q1_ref, g0_ref, g1_ref, *refs = refs
    part_refs, refs = refs[: chunks // 2], refs[chunks // 2 :]
    dq0_ref, dq1_ref, kv_buf, part_buf, sems, *refs = refs
    keys_buf, keys_t_buf, values_buf, key_acc, value_acc = refs

    def spot(place_ref, slot):
        at = place_ref[slot]
        return at // 2, at % 2

    loads = [pltpu.make_async_copy(ref, kv_buf.at[i], sems.at[i]) for i, ref in enumerate(kv_refs)]
    for i, load in enumerate(loads):
        pl.when(needed_ref[i] > 0)(load.start)
    part_buf[...] = jnp.zeros_like(part_buf)
    for i, load in enumerate(loads):
        pl.when(needed_ref[i] > 0)(load.wait)
    contract_last = (((1,), (1,)), ((), ()))
    for sub, (place_ref, q_ref, g_ref, hide_ref, dq_ref) in enumerate(
        (
            (place0_ref, q0_ref, g0_ref, hide0_ref, dq0_ref),
            (place1_ref, q1_ref, g1_ref, hide1_ref, dq1_ref),
        )
    ):
        for slot in range(pool):
            chunk, block = spot(place_ref, slot)
            rows = pl.ds(slot * BLK, BLK)
            keys_buf[sub, rows, :] = kv_buf[chunk, 0, block]
            values_buf[sub, rows, :] = kv_buf[chunk, 1, block]
        keys_t_buf[sub] = keys_buf[sub].T
        heads, tokens, head_dim = q_ref.shape
        query_rows = q_ref[...].reshape(heads * tokens, head_dim)
        upstream_rows = g_ref[...].reshape(heads * tokens, head_dim)
        hide = jnp.concatenate([hide_ref[...]] * heads, axis=1)
        scores = lax.dot_general(
            keys_buf[sub], query_rows, contract_last, preferred_element_type=jnp.float32
        )
        scores = scores * (scaling * math.log2(math.e)) + hide
        peak = jnp.max(scores, axis=0, keepdims=True)
        weights = jnp.exp2(scores - peak)
        total = jnp.sum(weights, axis=0, keepdims=True)
        slope = lax.dot_general(
            values_buf[sub], upstream_rows, contract_last, preferred_element_type=jnp.float32
        )
        share = 1.0 / total
        inner = jnp.sum(weights * slope, axis=0, keepdims=True) * share
        weights_low = (weights * share).astype(jnp.bfloat16)
        dscore = (weights * ((slope - inner) * (share * scaling))).astype(jnp.bfloat16)
        dquery_t = jnp.dot(keys_t_buf[sub], dscore, preferred_element_type=jnp.float32)
        dq_ref[...] = dquery_t.T.astype(jnp.bfloat16).reshape(heads, tokens, head_dim)
        key_acc[sub] = jnp.dot(dscore, query_rows, preferred_element_type=jnp.float32)
        value_acc[sub] = jnp.dot(weights_low, upstream_rows, preferred_element_type=jnp.float32)

    for kind, acc in enumerate((key_acc, value_acc)):
        for slot in range(pool):
            chunk, block = spot(place0_ref, slot)
            rows = pl.ds(slot * BLK, BLK)
            part_buf[chunk, kind, block] = acc[0, rows, :].astype(jnp.bfloat16)
        for slot in range(pool):
            chunk, block = spot(place1_ref, slot)
            twin = twin_ref[slot]
            rows = pl.ds(slot * BLK, BLK)
            twin_rows = pl.ds(pl.multiple_of(jnp.maximum(twin, 0) * BLK, BLK), BLK)
            shared = jnp.where(twin >= 0, acc[0, twin_rows, :], 0.0)
            part_buf[chunk, kind, block] = (acc[1, rows, :] + shared).astype(jnp.bfloat16)
    for i, ref in enumerate(part_refs):
        ref[...] = part_buf[2 * i : 2 * i + 2]


def placed(shape):
    return pltpu.VMEM(shape, jnp.bfloat16)


def attend(place0, place1, twin, needed, kv, hide0, hide1, q0, q1, g0, g1, pool):
    heads, tokens, head_dim = q0.shape
    keys = pool * BLK
    chunks = len(kv)
    scalar = pl.BlockSpec(memory_space=pltpu.SMEM)
    whole = pl.BlockSpec(memory_space=pltpu.VMEM)
    wide = [
        pltpu.with_memory_space_constraint(x, pltpu.VMEM) for x in (hide0, hide1, q0, q1, g0, g1)
    ]
    far = [pltpu.with_memory_space_constraint(x, pltpu.HBM) for x in kv]
    *part, dq0, dq1 = pl.pallas_call(
        functools.partial(
            attend_kernel, chunks=chunks, pool=pool, scaling=1.0 / math.sqrt(head_dim)
        ),
        in_specs=[scalar] * 4 + [pl.BlockSpec(memory_space=pltpu.HBM)] * chunks + [whole] * len(wide),
        out_specs=[whole] * (chunks // 2 + 2),
        scratch_shapes=[
            pltpu.VMEM((chunks, *kv[0].shape), jnp.bfloat16),
            pltpu.VMEM((chunks, *kv[0].shape), jnp.bfloat16),
            pltpu.SemaphoreType.DMA((chunks,)),
            pltpu.VMEM((2, keys, head_dim), jnp.bfloat16),
            pltpu.VMEM((2, head_dim, keys), jnp.bfloat16),
            pltpu.VMEM((2, keys, head_dim), jnp.bfloat16),
            pltpu.VMEM((2, keys, head_dim), jnp.float32),
            pltpu.VMEM((2, keys, head_dim), jnp.float32),
        ],
        out_shape=[
            *[placed((2, *x.shape)) for x in kv[::2]],
            placed(q0.shape),
            placed(q0.shape),
        ],
        compiler_params=pltpu.CompilerParams(vmem_limit_bytes=VMEM_LIMIT),
        cost_estimate=pl.CostEstimate(
            flops=2 * 5 * 2 * heads * tokens * keys * head_dim,
            bytes_accessed=16 * 2**20,
            transcendentals=2 * heads * tokens * keys,
        ),
    )(place0, place1, twin, needed, *far, *wide)
    return part, dq0, dq1


def choose_pool(chosen, device, core, chip, owners, own_blocks, fetched):
    tokens = chosen.shape[0]
    chips = owners // 2
    ids = jnp.arange(owners * own_blocks, dtype=jnp.int32)
    named = jnp.any(chosen.reshape(-1, 1) == ids[None, :], axis=0)
    far = named & (ids // own_blocks != device)
    rank = jnp.sum(jnp.where(far[:, None] & (ids[:, None] < ids[None, :]), 1, 0), axis=0)
    picker = far[None, :] & (rank[None, :] == jnp.arange(fetched, dtype=jnp.int32)[:, None])
    far_blocks = jnp.sum(jnp.where(picker, ids[None, :], 0), axis=1)
    blocks = jnp.concatenate([device * own_blocks + jnp.arange(own_blocks, dtype=jnp.int32), far_blocks])
    owner = blocks // own_blocks
    half = (owner % 2) ^ core
    away = (chip - owner // 2) % chips
    half_way = chips // 2
    chunk = jnp.where(away <= half_way, away, half_way + chips - away)
    place = (2 * chunk + half) * own_blocks + blocks % own_blocks
    picked = jnp.any(chosen[None, :, :] == blocks[:, None, None], axis=2)
    key_pos = blocks[:, None] * BLK + jnp.arange(BLK, dtype=jnp.int32)[None, :]
    query_pos = device * tokens + jnp.arange(tokens, dtype=jnp.int32)
    visible = picked[:, None, :] & (key_pos[:, :, None] <= query_pos[None, None, :])
    hide = jnp.where(visible, 0.0, -jnp.inf).astype(jnp.float32)
    return place, hide.reshape(-1, tokens)


def local(queries, keys, values, grad_out, selected):
    tokens, head_count, head_dim = queries.shape
    groups = keys.shape[1]
    per_group = head_count // groups
    own_blocks = tokens // BLK
    owners = lax.axis_size("ctx")
    chips = owners // 2
    half_way = chips // 2
    fetched = min(owners - 2, max(selected.shape[2] - own_blocks, 4)) + 1
    pool = own_blocks + fetched
    device = lax.axis_index("ctx").astype(jnp.int32)
    chip = device // 2
    core = device % 2
    first = core == 0

    def move(x, hops, change=False):
        pairs = []
        for src in range(owners):
            dst_core = (src % 2) ^ int(change)
            pairs.append((src, 2 * ((src // 2 + hops) % chips) + dst_core))
        return lax.ppermute(x, "ctx", pairs)

    def mine_other(zero, one):
        return jnp.where(first, zero, one), jnp.where(first, one, zero)

    kv0 = jnp.stack([keys[:, 0], values[:, 0]])
    kv1 = jnp.stack([keys[:, 1], values[:, 1]])
    kv_mine, kv_other = mine_other(kv0, kv1)

    kv_partner = move(kv_other, 0, True)
    ups = [(move(kv_mine, 1), move(kv_other, 1, True))]
    downs = [(move(kv_mine, -1), move(kv_other, -1, True))]
    for hop in range(1, half_way):
        ups.append(tuple(move(x, 1) for x in ups[-1]))
        if hop < half_way - 1:
            downs.append(tuple(move(x, -1) for x in downs[-1]))
    gathered = [x for pair in ((kv_mine, kv_partner), *ups, *downs) for x in pair]
    gathered = [x.reshape(2, own_blocks, BLK, head_dim) for x in gathered]

    def held(x, hop):
        return lax.optimization_barrier((x, ups[hop - 1][0]))[0]

    chosen = held(selected, 2)
    sel_mine, sel_other = mine_other(chosen[:, 0], chosen[:, 1])
    sel_partner = move(sel_other, 0, True)
    place0, hide0 = choose_pool(held(sel_mine, 7), device, core, chip, owners, own_blocks, fetched)
    place1, hide1 = choose_pool(held(sel_partner, 9), device ^ 1, core, chip, owners, own_blocks, fetched)
    same = place1[:, None] == place0[None, :]
    twin = jnp.max(jnp.where(same, jnp.arange(pool, dtype=jnp.int32)[None, :], -1), axis=1)

    chunk_ids = jnp.arange(len(gathered), dtype=jnp.int32)[:, None]
    named = jnp.concatenate([place0, place1])[None, :] // own_blocks == chunk_ids
    needed = jnp.any(named, axis=1).astype(jnp.int32)

    def split_heads(x):
        return mine_other(x[:, :per_group], x[:, per_group:])

    def heads_first(x):
        return x.transpose(1, 0, 2)

    q_mine, q_other = split_heads(held(queries, 3))
    g_mine, g_other = split_heads(held(grad_out, 5))
    q_partner = move(q_other, 0, True)
    g_partner = move(g_other, 0, True)

    part, dq_mine, dq_partner = attend(
        place0,
        place1,
        twin,
        needed,
        gathered,
        hide0,
        hide1,
        heads_first(q_mine),
        heads_first(q_partner),
        heads_first(g_mine),
        heads_first(g_partner),
        pool,
    )
    own, *part = [x.reshape(2, 2, tokens, head_dim) for x in part]
    f32 = jnp.float32

    def add(x, y):
        return (x.astype(f32) + y.astype(f32)).astype(jnp.bfloat16)

    down = part[half_way - 1]
    up = part[-1]
    for hop in range(half_way - 1, 0, -1):
        down = add(move(down, -1), part[hop - 1])
        if hop < half_way - 1:
            up = add(move(up, 1), part[half_way + hop - 1])
    grad_same = own[0].astype(f32) + move(down[0], -1).astype(f32) + move(up[0], 1).astype(f32)
    grad_cross = (
        move(own[1], 0, True).astype(f32)
        + move(down[1], -1, True).astype(f32)
        + move(up[1], 1, True).astype(f32)
    )
    zero, one = mine_other(grad_same, grad_cross)
    key_grad = jnp.stack([zero[0], one[0]], axis=1).astype(jnp.bfloat16)
    value_grad = jnp.stack([zero[1], one[1]], axis=1).astype(jnp.bfloat16)

    dq_other = move(dq_partner, 0, True)
    dq_zero, dq_one = mine_other(dq_mine, dq_other)
    dquery = jnp.concatenate([dq_zero, dq_one], axis=0).transpose(1, 0, 2)
    return (dquery, key_grad, value_grad)


def solution(mesh):
    spec = P(("rep", "ctx"), None, None)
    return jax.shard_map(
        local,
        mesh=mesh,
        in_specs=(spec,) * 5,
        out_specs=(spec,) * 3,
        check_vma=False,
    )
```
